32 devices in a mesh: rep: 4 (over x, y), dp: 8 (over z, core).
Axes of the slice: x: 2, y: 2, z: 4, core: 2. Of those that a mesh axis runs over, the one named last changes fastest.
Arguments:
- x: bfloat16 [32, 2048, 640], P(('rep', 'dp')), parts along dimension 0
- dy: bfloat16 [32, 2048, 640], P(('rep', 'dp')), parts along dimension 0
- w_gate: bfloat16 [2, 640, 2048], replicated
- w_up: bfloat16 [2, 640, 2048], replicated
- w_down: bfloat16 [2, 2048, 640], replicated
- m_w_gate: float32 [2, 640, 2048], P(None, 'dp')
- m_w_up: float32 [2, 640, 2048], P(None, 'dp')
- m_w_down: float32 [2, 2048, 640], P(None, 'dp')
- v_w_gate: float32 [2, 640, 2048], P(None, 'dp')
- v_w_up: float32 [2, 640, 2048], P(None, 'dp')
- v_w_down: float32 [2, 2048, 640], P(None, 'dp')
Outputs:
- output 1: bfloat16 [8, 640, 2048], P('rep'), parts along dimension 0
- output 2: bfloat16 [8, 640, 2048], P('rep'), parts along dimension 0
- output 3: bfloat16 [8, 2048, 640], P('rep'), parts along dimension 0
- output 4: float32 [8, 640, 2048], P('rep', 'dp'), parts along dimension 0
- output 5: float32 [8, 640, 2048], P('rep', 'dp'), parts along dimension 0
- output 6: float32 [8, 2048, 640], P('rep', 'dp'), parts along dimension 0
- output 7: float32 [8, 640, 2048], P('rep', 'dp'), parts along dimension 0
- output 8: float32 [8, 640, 2048], P('rep', 'dp'), parts along dimension 0
- output 9: float32 [8, 2048, 640], P('rep', 'dp'), parts along dimension 0
There are 4 independent parts. The reference program is written for one: setup_inputs(seed, part) draws one part's arguments, and reference() takes and returns one part's arrays. A program takes and returns all parts, laid end to end along the dimension named above; an argument that names none is the same for every part.
All inputs are finite; a program needn't handle non-finite values.
Results may differ from the reference program's by a relative error of at most 0.022.
Values are sent between devices in bfloat16 or wider.
A program may use at most 2 GiB of HBM per device.

```python
import jax
import jax.numpy as jnp
from jax import lax

SEQUENCES = 8
TOKENS = 2048
D = 640
FF = 2048
LAYERS = 2
NAMES = ("w_gate", "w_up", "w_down")
SHAPES = {"w_gate": (LAYERS, D, FF), "w_up": (LAYERS, D, FF), "w_down": (LAYERS, FF, D)}


def bump(key, n, height):
    away = (jnp.arange(n, dtype=jnp.int32) - jax.random.randint(key, (), 0, n, jnp.int32)) % n
    return jnp.where(away < n // 8, height, 1.0)


def together(key, own, strength):
    shared = jax.random.normal(key, own.shape[1:], jnp.float32)
    return (own + strength * shared) * lax.rsqrt(1 + strength * strength)


def setup_inputs(seed: int = 0, part: int = 0) -> dict:
    kx, kdy, ka, kb, kz, kf, kh, kl, *keys = jax.random.split(jax.random.key(seed), 8 + 3 * len(NAMES))
    kx, kdy, ka, kb = (jax.random.fold_in(k, part) for k in (kx, kdy, ka, kb))
    kw, km, kv = (keys[i::3] for i in range(3))
    shape = (SEQUENCES, TOKENS, D)
    much_x, much_dy = jax.random.uniform(kz, (2,), jnp.float32, 0.0, 1.0)
    loud = 2.0 ** jax.random.uniform(jax.random.fold_in(kz, 1), (), jnp.float32, -1.0, 2.0)
    layers = 2.0 ** jax.random.uniform(kl, (LAYERS, 1, 1), jnp.float32, -1.0, 1.0)
    x = together(ka, jax.random.normal(kx, shape, jnp.float32), much_x) * bump(kf, D, 4.0)
    dy = together(kb, jax.random.normal(kdy, shape, jnp.float32), much_dy)
    drawn = {"x": x.astype(jnp.bfloat16), "dy": (loud * dy * (SEQUENCES * TOKENS) ** -0.5).astype(jnp.bfloat16)}
    for key, name in zip(kw, NAMES, strict=True):
        w = jax.random.normal(key, SHAPES[name], jnp.float32) * SHAPES[name][1] ** -0.5
        drawn[name] = (w * {"w_gate": 1.0, "w_up": bump(kh, FF, 4.0), "w_down": layers}[name]).astype(jnp.bfloat16)
    for key, name in zip(km, NAMES, strict=True):
        drawn[f"m_{name}"] = 0.1 * jax.random.normal(key, SHAPES[name], jnp.float32)
    for key, name in zip(kv, NAMES, strict=True):
        drawn[f"v_{name}"] = jax.random.uniform(key, SHAPES[name], jnp.float32, 0.005, 0.015)
    return drawn


def matmul(a, w):
    return jnp.dot(a, w, preferred_element_type=jnp.float32).astype(jnp.bfloat16)


def normed(h):
    wide = h.astype(jnp.float32)
    scale = lax.rsqrt(jnp.mean(wide**2, -1, keepdims=True) + 1e-6)
    return (wide * scale).astype(jnp.bfloat16)


def layer(h, w):
    a = normed(h)
    gate = jnp.dot(a, w["w_gate"], preferred_element_type=jnp.float32)
    up = jnp.dot(a, w["w_up"], preferred_element_type=jnp.float32)
    return h + matmul((jax.nn.silu(gate) * up).astype(jnp.bfloat16), w["w_down"])


def adamw(w, m, v, g):
    m = 0.9 * m + 0.1 * g
    v = 0.95 * v + 0.05 * g * g
    step = m * lax.rsqrt(v + 1e-8) + 0.1 * w
    return (w - 0.02 * step).astype(jnp.bfloat16), m, v


def stack(weights, h):
    return lax.scan(lambda h, w: (layer(h, w), None), h, weights)[0]


def reference(x, dy, w_gate, w_up, w_down, m_w_gate, m_w_up, m_w_down, v_w_gate, v_w_up, v_w_down):
    weights = dict(zip(NAMES, (w_gate, w_up, w_down), strict=True))

    def take(so_far, sequence):
        h, by_y = sequence
        _, back = jax.vjp(lambda w: stack(w, h), weights)
        return jax.tree.map(lambda total, term: total + term.astype(jnp.float32), so_far, back(by_y)[0]), None

    none_yet = {name: jnp.zeros(w.shape, jnp.float32) for name, w in weights.items()}
    by_weights, _ = lax.scan(take, none_yet, (x, dy))
    gradients = [by_weights[name].astype(jnp.bfloat16).astype(jnp.float32) for name in NAMES]
    new = [
        adamw(w.astype(jnp.float32), m, v, g)
        for w, m, v, g in zip((w_gate, w_up, w_down), (m_w_gate, m_w_up, m_w_down), (v_w_gate, v_w_up, v_w_down), gradients, strict=True)
    ]
    return tuple(one[which] for which in range(3) for one in new)
```

```python
import functools

import jax
import jax.numpy as jnp
from jax import lax
from jax.experimental import pallas as pl
from jax.experimental.pallas import tpu as pltpu
from jax.sharding import PartitionSpec as P

D, FF, CHUNKS = 640, 2048, 16
BF, F32 = jnp.bfloat16, jnp.float32
SLOTS = 4


def normed(h):
    wide = h.astype(F32)
    scale = lax.rsqrt(jnp.mean(wide**2, -1, keepdims=True) + 1e-6)
    return (wide * scale).astype(BF)


def dot(a, b):
    return lax.dot_general(a, b, (((1,), (0,)), ((), ())), preferred_element_type=F32)


def dot_t(a, b):
    return lax.dot_general(a, b, (((1,), (1,)), ((), ())), preferred_element_type=F32)


def where(j):
    layer, s, h = 1 - j // 8, j % 4, (j // 4) % 2
    first = pl.multiple_of(s * 512 + h * 128, 128)
    return layer, s, h, first, pl.multiple_of(first + 256, 128)


def adam(w, m, v, g):
    m = 0.9 * m + 0.1 * g
    v = 0.95 * v + 0.05 * g * g
    return (w - 0.02 * (m * lax.rsqrt(v + 1e-8) + 0.1 * w)).astype(BF), m, v


def kernel(tile, a1, a0, h1, dy, wg, wu, wd, og, ou, od, mg, mu, md, vg, vu, vd,
           ng, nu, nd, pmg, pmu, pmd, pvg, pvu, pvd,
           a_s, at_s, do_s, dot_s, h_s, da_s, act_s, dg_s, du_s, wgb, wub, wdb, gg, gu, gd,
           pg, pd, d2s_g, d2s_d, d2r_g, d2r_d, sr_g, sr_d, sl_g, sl_d, rl_g, rl_d, rr_g, rr_d, nw_g, nw_d,
           wsem, lsem, d2_ss, d2_rs, sr_ss, rl_rs, sl_ss, rr_rs, own_s, ar_ss, al_ss, ap_ss, al_rs, ar_rs, ap_rs):
    dev = lax.axis_index("dp")
    z, k = dev // 2, dev % 2
    right, left, other = {"dp": (dev + 2) % 8}, {"dp": (dev + 6) % 8}, {"dp": z * 2 + 1 - k}
    tiles = a_s.shape[0] // tile

    barrier = pltpu.get_barrier_semaphore()
    for to in (right, left, other):
        pl.semaphore_signal(barrier, inc=1, device_id=to, device_id_type=pl.DeviceIdType.MESH)
    pl.semaphore_wait(barrier, 3)

    def remote(src, dst, ss, rs, to):
        return pltpu.make_async_remote_copy(src_ref=src, dst_ref=dst, send_sem=ss, recv_sem=rs, device_id=to,
                                            device_id_type=pl.DeviceIdType.MESH)

    def ok(j):
        return (j >= 0) & (j < CHUNKS)

    def weights(j):
        layer, _, _, c1, c2 = where(j)
        slot = j % 2
        out = []
        for i, c in enumerate((c1, c2)):
            here = slice(128 * i, 128 * i + 128)
            out.append((wg.at[layer, :, pl.ds(c, 128)], wgb.at[slot, :, here]))
            out.append((wu.at[layer, :, pl.ds(c, 128)], wub.at[slot, :, here]))
            out.append((wd.at[layer, pl.ds(c, 128), :], wdb.at[slot, here, :]))
        return [pltpu.make_async_copy(src, dst, wsem.at[slot, i]) for i, (src, dst) in enumerate(out)]

    def over_tiles(body):
        @pl.loop(0, tiles)
        def _(i):
            body(pl.ds(pl.multiple_of(i * tile, tile), tile))

    first = [pltpu.make_async_copy(a1, a_s, lsem.at[0]), pltpu.make_async_copy(dy, do_s, lsem.at[1]),
             pltpu.make_async_copy(h1, h_s, lsem.at[2])]
    for c in first + weights(0):
        c.start()
    for c in first:
        c.wait()

    def chunk(t):
        slot = t % 2

        @pl.when(t == 8)
        def _():
            fetch = pltpu.make_async_copy(a0, a_s, lsem.at[0])
            fetch.start()

            def back(rows):
                h = h_s[rows, :].astype(F32)
                da = da_s[rows, :].astype(BF).astype(F32)
                r = lax.rsqrt(jnp.mean(h * h, -1, keepdims=True) + 1e-6)
                dh = r * da - h * (r * r * r * jnp.mean(h * da, -1, keepdims=True))
                do_s[rows, :] = (do_s[rows, :].astype(F32) + dh.astype(BF).astype(F32)).astype(BF)

            over_tiles(back)
            fetch.wait()

        @pl.when((t == 0) | (t == 8))
        def _():
            def turn(rows):
                at_s[:, rows] = a_s[rows, :].T
                dot_s[:, rows] = do_s[rows, :].T
                da_s[rows, :] = jnp.zeros((tile, D), F32)

            over_tiles(turn)

        for c in weights(t):
            c.wait()

        @pl.when(t + 1 < CHUNKS)
        def _():
            for c in weights(t + 1):
                c.start()

        def through(rows):
            a, d = a_s[rows, :], do_s[rows, :]
            gate, up = dot(a, wgb[slot]), dot(a, wub[slot])
            dact = dot_t(d, wdb[slot]).astype(BF).astype(F32)
            sig = jax.nn.sigmoid(gate)
            silu = gate * sig
            act_s[rows, :] = (silu * up).astype(BF)
            du_s[rows, :] = (dact * silu).astype(BF)
            dg_s[rows, :] = (dact * up * (sig * (1 + gate * (1 - sig)))).astype(BF)

        over_tiles(through)

        @pl.when(t < 8)
        def _():
            def into(rows):
                da_s[rows, :] += dot_t(dg_s[rows, :], wgb[slot]) + dot_t(du_s[rows, :], wub[slot])

            over_tiles(into)

    def gradients(t):
        slot, keep = t % 2, t % SLOTS
        gg[...] = dot(at_s[...], dg_s[...])
        gu[...] = dot(at_s[...], du_s[...])
        gd[...] = dot(dot_s[...], act_s[...])
        for b in range(4):
            mine = pl.ds(pl.multiple_of(160 * b + 80 * k, 16), 80)
            its = pl.ds(pl.multiple_of(160 * b + 80 * (1 - k), 16), 80)
            for i, g in enumerate((gg, gu)):
                pg[keep, b, 80 * i : 80 * i + 80, :] = g[mine, :]
                d2s_g[slot, b, 80 * i : 80 * i + 80, :] = g[its, :].astype(BF)
        pd[keep] = gd[:, pl.ds(pl.multiple_of(128 * k, 128), 128)].T
        d2s_d[slot] = gd[:, pl.ds(pl.multiple_of(128 * (1 - k), 128), 128)].T.astype(BF)
        for c in swap(t):
            c.start()

    def swap(j):
        slot, keep = j % 2, j % SLOTS
        return [remote(d2s_g.at[slot], d2r_g.at[keep], d2_ss.at[slot, 0], d2_rs.at[keep, 0], other),
                remote(d2s_d.at[slot], d2r_d.at[keep], d2_ss.at[slot, 1], d2_rs.at[keep, 1], other)]

    def to_right(j, b):
        return remote(sr_g.at[j % 2, b - 1], rl_g.at[j % SLOTS, b - 1], sr_ss.at[j % 2, b - 1], rl_rs.at[j % SLOTS, b - 1], right)

    def to_right_d(j):
        return remote(sr_d.at[j % 2], rl_d.at[j % SLOTS], sr_ss.at[j % 2, 3], rl_rs.at[j % SLOTS, 3], right)

    def to_left(j, b):
        return remote(sl_g.at[j % 2, b], rr_g.at[j % SLOTS, b], sl_ss.at[j % 2, b], rr_rs.at[j % SLOTS, b], left)

    def to_left_d(j):
        return remote(sl_d.at[j % 2], rr_d.at[j % SLOTS], sl_ss.at[j % 2, 3], rr_rs.at[j % SLOTS, 3], left)

    def reduce(t):
        j = t - 1

        @pl.when(ok(j))
        def _():
            for c in swap(j):
                c.wait()
            keep = j % SLOTS
            for b in range(4):
                pg[keep, b] += d2r_g[keep, b].astype(F32)
            pd[keep] += d2r_d[keep].astype(F32)

        def rightward(j, act):
            s = where(j)[1]
            for b in (1, 2, 3):
                pl.when(ok(j) & (z < b) & (z < 3))(lambda b=b: act(b))
            pl.when(ok(j) & (z < 3) & (z < s))(lambda: act(None))

        def leftward(j, act):
            s = where(j)[1]
            for b in (0, 1, 2):
                pl.when(ok(j) & (z > b) & (z > 0))(lambda b=b: act(b))
            pl.when(ok(j) & (z > 0) & (z > s))(lambda: act(None))

        jr = t - 1 - z
        s = where(jr)[1]
        for b in (1, 2, 3):
            @pl.when(ok(jr) & (z > 0) & (z <= b))
            def _():
                to_right(jr, b).wait_recv()
                pg[jr % SLOTS, b] += rl_g[jr % SLOTS, b - 1].astype(F32)

        @pl.when(ok(jr) & (z > 0) & (z <= s))
        def _():
            to_right_d(jr).wait_recv()
            pd[jr % SLOTS] += rl_d[jr % SLOTS].astype(F32)

        def send_r(b):
            if b is None:
                sr_d[jr % 2] = pd[jr % SLOTS].astype(BF)
                to_right_d(jr).start()
            else:
                sr_g[jr % 2, b - 1] = pg[jr % SLOTS, b].astype(BF)
                to_right(jr, b).start()

        rightward(jr, send_r)
        rightward(jr - 1, lambda b: (to_right_d(jr - 1) if b is None else to_right(jr - 1, b)).wait_send())

        jl = t - 4 + z
        s = where(jl)[1]
        for b in (0, 1, 2):
            @pl.when(ok(jl) & (z < 3) & (z >= b))
            def _():
                to_left(jl, b).wait_recv()
                pg[jl % SLOTS, b] += rr_g[jl % SLOTS, b].astype(F32)

        @pl.when(ok(jl) & (z < 3) & (z >= s))
        def _():
            to_left_d(jl).wait_recv()
            pd[jl % SLOTS] += rr_d[jl % SLOTS].astype(F32)

        def send_l(b):
            if b is None:
                sl_d[jl % 2] = pd[jl % SLOTS].astype(BF)
                to_left_d(jl).start()
            else:
                sl_g[jl % 2, b] = pg[jl % SLOTS, b].astype(BF)
                to_left(jl, b).start()

        leftward(jl, send_l)
        leftward(jl - 1, lambda b: (to_left_d(jl - 1) if b is None else to_left(jl - 1, b)).wait_send())

    def update(j):
        layer, s, h, c1, c2 = where(j)
        keep, slot = j % SLOTS, j % 2
        for i, (w, m, v, pm, pv) in enumerate(((og, mg, vg, pmg, pvg), (ou, mu, vu, pmu, pvu))):
            for n, c in enumerate((c1, c2)):
                at = (layer, slice(None), pl.ds(c, 128))
                g = pg[keep, z, 80 * i : 80 * i + 80, 128 * n : 128 * n + 128].astype(BF).astype(F32)
                new, pm[at], pv[at] = adam(w[at].astype(F32), m[at], v[at], g)
                nw_g[slot, 80 * i : 80 * i + 80, 128 * n : 128 * n + 128] = new

        @pl.when(s == z)
        def _():
            at = (layer, pl.ds(pl.multiple_of(h * 128, 128), 128), slice(None))
            g = pd[keep].astype(BF).astype(F32)
            new, pmd[at], pvd[at] = adam(od[at].astype(F32), md[at], vd[at], g)
            nw_d[slot] = new

    def windows(j, origin, core):
        layer, s, h, c1, c2 = where(j)
        rows = pl.ds(pl.multiple_of(160 * origin + 80 * core, 16), 80)
        down = pl.ds(pl.multiple_of((2 * origin + core) * 256 + 128 * h, 128), 128)
        return [n.at[layer, rows, pl.ds(c, 128)] for n in (ng, nu) for c in (c1, c2)], nd.at[layer, down, :], s == origin

    def sources(j, a, origin):
        if a == 0:
            slot = j % 2
            return [nw_g.at[slot, 80 * i : 80 * i + 80, 128 * n : 128 * n + 128] for i in range(2) for n in range(2)], nw_d.at[slot]
        return windows(j, origin, k)[:2]

    def start(j, a, origin, ss, rs, to):
        into, into_d, has = windows(j, origin, k)
        src, src_d = sources(j, a, origin)
        for x, y in zip(src, into, strict=True):
            remote(x, y, ss.at[j % 2, a, 0], rs.at[j % SLOTS, a, 0], to).start()

        @pl.when(has)
        def _():
            remote(src_d, into_d, ss.at[j % 2, a, 1], rs.at[j % SLOTS, a, 1], to).start()

    def finish(has, gate_up, down):
        pltpu.make_async_copy(nw_g.at[0], nw_g.at[0], gate_up).wait()

        @pl.when(has)
        def _():
            pltpu.make_async_copy(nw_d.at[0], nw_d.at[0], down).wait()

    def gather(t):
        def each(j, a, origin, side, what):
            valid = ok(j) & (origin >= 0) & (origin < 4)
            has = where(j)[1] == origin

            @pl.when(valid)
            def _():
                if side in (0, 1) and a < 3:
                    pl.when(z < 3)(lambda: what(j, a, origin, has, ar_ss, al_rs, right))
                if side in (0, 2) and a < 3:
                    pl.when(z > 0)(lambda: what(j, a, origin, has, al_ss, ar_rs, left))
                what(j, a, origin, has, ap_ss.at[side], ap_rs.at[side], other)

        def waited(j, a, origin, has, ss, rs, to):
            finish(has, ss.at[j % 2, a, 0], ss.at[j % 2, a, 1])

        def begun(j, a, origin, has, ss, rs, to):
            start(j, a, origin, ss, rs, to)

        j = t - 4

        @pl.when(ok(j - 1))
        def _():
            finish(where(j - 1)[1] == z, own_s.at[(j - 1) % 2, 0], own_s.at[(j - 1) % 2, 1])

        each(j - 1, 0, z, 0, waited)

        @pl.when(ok(j))
        def _():
            update(j)
            into, into_d, has = windows(j, z, k)
            src, src_d = sources(j, 0, z)
            for x, y in zip(src, into, strict=True):
                pltpu.make_async_copy(x, y, own_s.at[j % 2, 0]).start()

            @pl.when(has)
            def _():
                pltpu.make_async_copy(src_d, into_d, own_s.at[j % 2, 1]).start()

        each(j, 0, z, 0, begun)

        for a in (1, 2, 3):
            ja = t - 4 - a
            for side, origin, rs in ((1, z - a, al_rs), (2, z + a, ar_rs)):
                each(ja - 1, a, origin, side, waited)

                @pl.when(ok(ja) & (origin >= 0) & (origin < 4))
                def _():
                    finish(where(ja)[1] == origin, rs.at[ja % SLOTS, a - 1, 0], rs.at[ja % SLOTS, a - 1, 1])

                each(ja, a, origin, side, begun)

        for a in (0, 1, 2, 3):
            jp = t - 5 - a
            for side, origin in ((0, z),) if a == 0 else ((1, z - a), (2, z + a)):
                @pl.when(ok(jp) & (origin >= 0) & (origin < 4))
                def _():
                    finish(where(jp)[1] == origin, ap_rs.at[side, jp % SLOTS, a, 0], ap_rs.at[side, jp % SLOTS, a, 1])

    @pl.loop(0, CHUNKS + 8)
    def _(t):
        pl.when(t < CHUNKS)(lambda: chunk(t))
        reduce(t)
        gather(t)
        pl.when(t < CHUNKS)(lambda: gradients(t))


def step_kernel(tokens):
    tile = min(tokens, 512)
    sds = jax.ShapeDtypeStruct
    hbm, vmem = pl.BlockSpec(memory_space=pltpu.HBM), pl.BlockSpec(memory_space=pltpu.VMEM)
    wide, tall, block, down = (2, D, FF), (2, FF, D), (2, D // 8, FF), (2, FF // 8, D)
    gu, dn = (160, 256), (128, D)
    V, dma = pltpu.VMEM, pltpu.SemaphoreType.DMA
    scratch = [
        V((tokens, D), BF), V((D, tokens), BF), V((tokens, D), BF), V((D, tokens), BF), V((tokens, D), BF), V((tokens, D), F32),
        V((tokens, 256), BF), V((tokens, 256), BF), V((tokens, 256), BF),
        V((2, D, 256), BF), V((2, D, 256), BF), V((2, 256, D), BF), V((D, 256), F32), V((D, 256), F32), V((D, 256), F32),
        V((SLOTS, 4, *gu), F32), V((SLOTS, *dn), F32), V((2, 4, *gu), BF), V((2, *dn), BF), V((SLOTS, 4, *gu), BF), V((SLOTS, *dn), BF),
        V((2, 3, *gu), BF), V((2, *dn), BF), V((2, 3, *gu), BF), V((2, *dn), BF),
        V((SLOTS, 3, *gu), BF), V((SLOTS, *dn), BF), V((SLOTS, 3, *gu), BF), V((SLOTS, *dn), BF),
        V((2, *gu), BF), V((2, *dn), BF),
        dma((2, 6)), dma((3,)), dma((2, 2)), dma((SLOTS, 2)), dma((2, 4)), dma((SLOTS, 4)), dma((2, 4)), dma((SLOTS, 4)),
        dma((2, 2)), dma((2, 3, 2)), dma((2, 3, 2)), dma((3, 2, 4, 2)), dma((SLOTS, 3, 2)), dma((SLOTS, 3, 2)), dma((3, SLOTS, 4, 2)),
    ]
    return pl.pallas_call(
        functools.partial(kernel, tile),
        out_shape=[sds(wide, BF), sds(wide, BF), sds(tall, BF)] + [sds(s, F32) for s in (block, block, down)] * 2,
        in_specs=[hbm] * 7 + [vmem] * 9,
        out_specs=[hbm] * 3 + [vmem] * 6,
        scratch_shapes=scratch,
        compiler_params=pltpu.CompilerParams(collective_id=0, has_side_effects=True, vmem_limit_bytes=64 * 2**20),
        name="step",
    )


def solution(mesh):
    def step(x, dy, wg, wu, wd, *moments):
        x, dy = x[0], dy[0]
        a0 = normed(x)
        gate = dot(a0, wg[0])
        up = dot(a0, wu[0])
        h1 = x + dot((jax.nn.silu(gate) * up).astype(BF), wd[0]).astype(BF)
        a1 = normed(h1)
        me = lax.axis_index("dp")
        own = [lax.dynamic_slice_in_dim(w, me * (w.shape[1] // 8), w.shape[1] // 8, 1) for w in (wg, wu, wd)]
        return tuple(step_kernel(x.shape[0])(a1, a0, h1, dy, wg, wu, wd, *own, *moments))

    mine, whole, rows = P(("rep", "dp"), None, None), P(None, None, None), P(None, "dp", None)
    return jax.shard_map(
        step, mesh=mesh, in_specs=(mine, mine) + (whole,) * 3 + (rows,) * 6,
        out_specs=(P("rep", None, None),) * 3 + (P("rep", "dp", None),) * 6, check_vma=False,
    )
```

```python
import functools

import jax
import jax.numpy as jnp
from jax import lax
from jax.experimental import pallas as pl
from jax.experimental.pallas import tpu as pltpu
from jax.sharding import PartitionSpec as P

D, FF, CHUNKS = 640, 2048, 16
BF, F32 = jnp.bfloat16, jnp.float32
SLOTS = 4
HELD = 5


def dot(a, b):
    return lax.dot_general(a, b, (((1,), (0,)), ((), ())), preferred_element_type=F32)


def dot_t(a, b):
    return lax.dot_general(a, b, (((1,), (1,)), ((), ())), preferred_element_type=F32)


def where(j):
    layer, h = 1 - j // 8, j % 2
    c1 = chip_of(j, 0) * 512 + h * 128
    c2 = chip_of(j, 1) * 512 + 256 + h * 128
    return layer, h, pl.multiple_of(c1, 128), pl.multiple_of(c2, 128)


def chip_of(j, core):
    s = (j // 2 + 3 - 2 * (j // 8)) % 4
    return s + core * (3 - 2 * s)


def adam(w, m, v, g):
    m = 0.9 * m + 0.1 * g
    v = 0.95 * v + 0.05 * g * g
    return (w - 0.02 * (m * lax.rsqrt(v + 1e-8) + 0.1 * w)).astype(BF), m, v


def kernel(tile, x, dy, wg, wu, wd, *refs):
    moments, (ng, nu, nd), new_moments, (a_s, at_s, do_s, dot_s, h_s, da_s, act_s, dg_s, du_s, wgb, wub, wdb, gg, gu, gd,
           pg, pd, d2s_g, d2s_d, d2r_g, d2r_d, sr_g, sr_d, sl_g, sl_d, rl_g, rl_d, rr_g, rr_d, nw_g, nw_d,
           og, ou, od, wsem, lsem, d2_ss, d2_rs, sr_ss, rl_rs, sl_ss, rr_rs, own_s, ar_ss, al_ss, ap_ss, al_rs, ar_rs, ap_rs,
           mg, mu, md, vg, vu, vd, msem) = refs[:6], refs[6:9], refs[9:15], refs[15:]
    held = (mg, mu, md, vg, vu, vd)
    dev = lax.axis_index("dp")
    z, k = dev // 2, dev % 2
    right, left, other = {"dp": (dev + 2) % 8}, {"dp": (dev + 6) % 8}, {"dp": z * 2 + 1 - k}
    tiles = h_s.shape[0] // tile

    barrier = pltpu.get_barrier_semaphore()
    for to in (right, left, other):
        pl.semaphore_signal(barrier, inc=1, device_id=to, device_id_type=pl.DeviceIdType.MESH)
    pl.semaphore_wait(barrier, 3)

    def remote(src, dst, ss, rs, to):
        return pltpu.make_async_remote_copy(src_ref=src, dst_ref=dst, send_sem=ss, recv_sem=rs, device_id=to,
                                            device_id_type=pl.DeviceIdType.MESH)

    def ok(j):
        return (j >= 0) & (j < CHUNKS)

    def weights(j):
        layer, _, c1, c2 = where(j)
        slot = j % 2
        out = []
        for i, c in enumerate((c1, c2)):
            here = slice(128 * i, 128 * i + 128)
            out.append((wg.at[layer, :, pl.ds(c, 128)], wgb.at[slot, :, here]))
            out.append((wu.at[layer, :, pl.ds(c, 128)], wub.at[slot, :, here]))
            out.append((wd.at[layer, pl.ds(c, 128), :], wdb.at[slot, here, :]))
        return [pltpu.make_async_copy(src, dst, wsem.at[slot, i]) for i, (src, dst) in enumerate(out)]

    def over_tiles(body):
        @pl.loop(0, tiles)
        def _(i):
            body(pl.ds(pl.multiple_of(i * tile, tile), tile))

    def unit(h):
        return lax.rsqrt(jnp.mean(h * h, -1, keepdims=True) + 1e-6)

    here = pltpu.make_async_copy(x, h_s, lsem.at[0])
    mine = pl.ds(pl.multiple_of(80 * dev, 16), 80)
    later = [pltpu.make_async_copy(wg.at[:, mine, :], og, lsem.at[2]), pltpu.make_async_copy(wu.at[:, mine, :], ou, lsem.at[3]),
             pltpu.make_async_copy(wd.at[:, pl.ds(pl.multiple_of(256 * dev, 256), 256), :], od, lsem.at[4]),
             pltpu.make_async_copy(dy, do_s, lsem.at[1])]
    later += [pltpu.make_async_copy(src, dst, msem.at[i]) for i, (src, dst) in enumerate(zip(moments, held, strict=True))]
    for c in [here] + weights(8) + later:
        c.start()
    here.wait()

    def enter(rows):
        h = h_s[rows, :].astype(F32)
        a_s[0, rows, :] = (h * unit(h)).astype(BF)
        da_s[rows, :] = jnp.zeros((tile, D), F32)

    over_tiles(enter)

    @pl.loop(8, 16)
    def _(j):
        slot = j % 2
        for c in weights(j):
            c.wait()
        for c in weights((j + 1) % 16):
            c.start()

        def forward(rows):
            a = a_s[0, rows, :]
            gate, up = dot(a, wgb[slot]), dot(a, wub[slot])
            da_s[rows, :] += dot((gate * jax.nn.sigmoid(gate) * up).astype(BF), wdb[slot])

        over_tiles(forward)

    def leave(rows):
        h = (h_s[rows, :].astype(F32) + da_s[rows, :].astype(BF).astype(F32)).astype(BF)
        h_s[rows, :] = h
        h = h.astype(F32)
        a_s[1, rows, :] = (h * unit(h)).astype(BF)
        at_s[1, :, rows] = a_s[1, rows, :].T
        dot_s[:, rows] = do_s[rows, :].T
        da_s[rows, :] = jnp.zeros((tile, D), F32)

    for c in later:
        c.wait()
    over_tiles(leave)

    def chunk(t):
        slot, layer = t % 2, 1 - t // 8

        @pl.when(t == 8)
        def _():
            def back(rows):
                h = h_s[rows, :].astype(F32)
                da = da_s[rows, :].astype(BF).astype(F32)
                r = unit(h)
                dh = r * da - h * (r * r * r * jnp.mean(h * da, -1, keepdims=True))
                do_s[rows, :] = (do_s[rows, :].astype(F32) + dh.astype(BF).astype(F32)).astype(BF)
                dot_s[:, rows] = do_s[rows, :].T

            over_tiles(back)

        @pl.when(t == 4)
        def _():
            def turn(rows):
                at_s[0, :, rows] = a_s[0, rows, :].T

            over_tiles(turn)

        for c in weights(t):
            c.wait()

        @pl.when(t + 1 < CHUNKS)
        def _():
            for c in weights(t + 1):
                c.start()

        def through(rows):
            a, d = a_s[layer, rows, :], do_s[rows, :]
            gate, up = dot(a, wgb[slot]), dot(a, wub[slot])
            dact = dot_t(d, wdb[slot]).astype(BF).astype(F32)
            sig = jax.nn.sigmoid(gate)
            silu = gate * sig
            act_s[rows, :] = (silu * up).astype(BF)
            du_s[rows, :] = (dact * silu).astype(BF)
            dg_s[rows, :] = (dact * up * (sig * (1 + gate * (1 - sig)))).astype(BF)

        over_tiles(through)

        @pl.when(t < 8)
        def _():
            def into(rows):
                da_s[rows, :] += dot_t(dg_s[rows, :], wgb[slot]) + dot_t(du_s[rows, :], wub[slot])

            over_tiles(into)

    def gradients(t):
        slot, keep, layer = t % 2, t % HELD, 1 - t // 8
        gg[...] = dot(at_s[layer], dg_s[...])
        gu[...] = dot(at_s[layer], du_s[...])
        gd[...] = dot(dot_s[...], act_s[...])
        for b in range(4):
            mine = pl.ds(pl.multiple_of(160 * b + 80 * k, 16), 80)
            its = pl.ds(pl.multiple_of(160 * b + 80 * (1 - k), 16), 80)
            for i, g in enumerate((gg, gu)):
                pg[keep, b, 80 * i : 80 * i + 80, :] = g[mine, :]
                d2s_g[slot, b, 80 * i : 80 * i + 80, :] = g[its, :].astype(BF)
        pd[keep] = gd[:, pl.ds(pl.multiple_of(128 * k, 128), 128)].T
        d2s_d[slot] = gd[:, pl.ds(pl.multiple_of(128 * (1 - k), 128), 128)].T.astype(BF)
        for c in swap(t):
            c.start()

    def swap(j):
        slot, keep = j % 2, j % SLOTS
        return [remote(d2s_g.at[slot], d2r_g.at[keep], d2_ss.at[slot, 0], d2_rs.at[keep, 0], other),
                remote(d2s_d.at[slot], d2r_d.at[keep], d2_ss.at[slot, 1], d2_rs.at[keep, 1], other)]

    def to_right(j, b):
        return remote(sr_g.at[j % 2, b - 1], rl_g.at[j % SLOTS, b - 1], sr_ss.at[j % 2, b - 1], rl_rs.at[j % SLOTS, b - 1], right)

    def to_right_d(j):
        return remote(sr_d.at[j % 2], rl_d.at[j % SLOTS], sr_ss.at[j % 2, 3], rl_rs.at[j % SLOTS, 3], right)

    def to_left(j, b):
        return remote(sl_g.at[j % 2, b], rr_g.at[j % SLOTS, b], sl_ss.at[j % 2, b], rr_rs.at[j % SLOTS, b], left)

    def to_left_d(j):
        return remote(sl_d.at[j % 2], rr_d.at[j % SLOTS], sl_ss.at[j % 2, 3], rr_rs.at[j % SLOTS, 3], left)

    def reduce(t):
        j = t - 1

        @pl.when(ok(j))
        def _():
            for c in swap(j):
                c.wait()
            keep, came = j % HELD, j % SLOTS
            for b in range(4):
                pg[keep, b] += d2r_g[came, b].astype(F32)
            pd[keep] += d2r_d[came].astype(F32)

        jr, jl = t - 1 - z, t - 4 + z
        sr, sl = chip_of(jr, k), chip_of(jl, k)

        def rightward(b):
            @pl.when(ok(jr) & (z > 0) & (z <= b))
            def _():
                to_right(jr, b).wait_recv()
                pg[jr % HELD, b] += rl_g[jr % SLOTS, b - 1].astype(F32)

            @pl.when(ok(jr) & (z < b))
            def _():
                sr_g[jr % 2, b - 1] = pg[jr % HELD, b].astype(BF)
                to_right(jr, b).start()

            @pl.when(ok(jr - 1) & (z < b))
            def _():
                to_right(jr - 1, b).wait_send()

        def leftward(b):
            @pl.when(ok(jl) & (z < 3) & (z >= b))
            def _():
                to_left(jl, b).wait_recv()
                pg[jl % HELD, b] += rr_g[jl % SLOTS, b].astype(F32)

            @pl.when(ok(jl) & (z > b))
            def _():
                sl_g[jl % 2, b] = pg[jl % HELD, b].astype(BF)
                to_left(jl, b).start()

            @pl.when(ok(jl - 1) & (z > b))
            def _():
                to_left(jl - 1, b).wait_send()

        for b in (3, 2, 1):
            rightward(b)
            leftward(3 - b)

        @pl.when(ok(jr) & (z > 0) & (z <= sr))
        def _():
            to_right_d(jr).wait_recv()
            pd[jr % HELD] += rl_d[jr % SLOTS].astype(F32)

        @pl.when(ok(jr) & (z < sr))
        def _():
            sr_d[jr % 2] = pd[jr % HELD].astype(BF)
            to_right_d(jr).start()

        @pl.when(ok(jr - 1) & (z < chip_of(jr - 1, k)))
        def _():
            to_right_d(jr - 1).wait_send()

        @pl.when(ok(jl) & (z < 3) & (z >= sl))
        def _():
            to_left_d(jl).wait_recv()
            pd[jl % HELD] += rr_d[jl % SLOTS].astype(F32)

        @pl.when(ok(jl) & (z > sl))
        def _():
            sl_d[jl % 2] = pd[jl % HELD].astype(BF)
            to_left_d(jl).start()

        @pl.when(ok(jl - 1) & (z > chip_of(jl - 1, k)))
        def _():
            to_left_d(jl - 1).wait_send()

    def update(j):
        layer, h, c1, c2 = where(j)
        keep, slot = j % HELD, j % 2
        for i, (w, m, v) in enumerate(((og, mg, vg), (ou, mu, vu))):
            for n, c in enumerate((c1, c2)):
                at = (layer, slice(None), pl.ds(c, 128))
                g = pg[keep, z, 80 * i : 80 * i + 80, 128 * n : 128 * n + 128].astype(BF).astype(F32)
                new, m[at], v[at] = adam(w[at].astype(F32), m[at], v[at], g)
                nw_g[slot, 80 * i : 80 * i + 80, 128 * n : 128 * n + 128] = new

        @pl.when(chip_of(j, k) == z)
        def _():
            at = (layer, pl.ds(pl.multiple_of(h * 128, 128), 128), slice(None))
            g = pd[keep].astype(BF).astype(F32)
            new, md[at], vd[at] = adam(od[at].astype(F32), md[at], vd[at], g)
            nw_d[slot] = new

    def windows(j, origin, core):
        layer, h, c1, c2 = where(j)
        rows = pl.ds(pl.multiple_of(160 * origin + 80 * core, 16), 80)
        down = pl.ds(pl.multiple_of((2 * origin + core) * 256 + 128 * h, 128), 128)
        return [n.at[layer, rows, pl.ds(c, 128)] for n in (ng, nu) for c in (c1, c2)], nd.at[layer, down, :], chip_of(j, core) == origin

    def sources(j, a, origin):
        if a == 0:
            slot = j % 2
            return [nw_g.at[slot, 80 * i : 80 * i + 80, 128 * n : 128 * n + 128] for i in range(2) for n in range(2)], nw_d.at[slot]
        return windows(j, origin, k)[:2]

    def start(j, a, origin, ss, rs, to):
        into, into_d, has = windows(j, origin, k)
        src, src_d = sources(j, a, origin)
        for x, y in zip(src, into, strict=True):
            remote(x, y, ss.at[j % 2, a, 0], rs.at[j % SLOTS, a, 0], to).start()

        @pl.when(has)
        def _():
            remote(src_d, into_d, ss.at[j % 2, a, 1], rs.at[j % SLOTS, a, 1], to).start()

    def finish(has, gate_up, down):
        pltpu.make_async_copy(nw_g.at[0], nw_g.at[0], gate_up).wait()

        @pl.when(has)
        def _():
            pltpu.make_async_copy(nw_d.at[0], nw_d.at[0], down).wait()

    def gather(t):
        def each(j, a, origin, side, what):
            valid = ok(j) & (origin >= 0) & (origin < 4)
            has = chip_of(j, k) == origin

            @pl.when(valid)
            def _():
                if side in (0, 1) and a < 3:
                    pl.when(z < 3)(lambda: what(j, a, origin, has, ar_ss, al_rs, right))
                if side in (0, 2) and a < 3:
                    pl.when(z > 0)(lambda: what(j, a, origin, has, al_ss, ar_rs, left))
                what(j, a, origin, has, ap_ss.at[side], ap_rs.at[side], other)

        def waited(j, a, origin, has, ss, rs, to):
            finish(has, ss.at[j % 2, a, 0], ss.at[j % 2, a, 1])

        def begun(j, a, origin, has, ss, rs, to):
            start(j, a, origin, ss, rs, to)

        j = t - 4

        @pl.when(ok(j - 1))
        def _():
            finish(chip_of(j - 1, k) == z, own_s.at[(j - 1) % 2, 0], own_s.at[(j - 1) % 2, 1])

        each(j - 1, 0, z, 0, waited)

        @pl.when(ok(j))
        def _():
            update(j)
            into, into_d, has = windows(j, z, k)
            src, src_d = sources(j, 0, z)
            for x, y in zip(src, into, strict=True):
                pltpu.make_async_copy(x, y, own_s.at[j % 2, 0]).start()

            @pl.when(has)
            def _():
                pltpu.make_async_copy(src_d, into_d, own_s.at[j % 2, 1]).start()

        each(j, 0, z, 0, begun)

        for a in (1, 2, 3):
            ja = t - 4 - a
            for side, origin, rs in ((1, z - a, al_rs), (2, z + a, ar_rs)):
                each(ja - 1, a, origin, side, waited)

                @pl.when(ok(ja) & (origin >= 0) & (origin < 4))
                def _():
                    finish(chip_of(ja, k) == origin, rs.at[ja % SLOTS, a - 1, 0], rs.at[ja % SLOTS, a - 1, 1])

                each(ja, a, origin, side, begun)

        for a in (0, 1, 2, 3):
            jp = t - 5 - a
            for side, origin in ((0, z),) if a == 0 else ((1, z - a), (2, z + a)):
                @pl.when(ok(jp) & (origin >= 0) & (origin < 4))
                def _():
                    finish(chip_of(jp, 1 - k) == origin, ap_rs.at[side, jp % SLOTS, a, 0], ap_rs.at[side, jp % SLOTS, a, 1])

    back_out = [pltpu.make_async_copy(src, dst, msem.at[i]) for i, (src, dst) in enumerate(zip(held, new_moments, strict=True))]

    @pl.loop(0, CHUNKS + 8)
    def _(t):
        pl.when(t < CHUNKS)(lambda: chunk(t))
        reduce(t)
        pl.when(t < CHUNKS)(lambda: gradients(t))
        gather(t)

        @pl.when(t == CHUNKS + 3)
        def _():
            for c in back_out:
                c.start()

    for c in back_out:
        c.wait()


def step_kernel(tokens):
    tile = min(tokens, 1024)
    sds = jax.ShapeDtypeStruct
    hbm = pl.BlockSpec(memory_space=pltpu.HBM)
    wide, tall, block, down = (2, D, FF), (2, FF, D), (2, D // 8, FF), (2, FF // 8, D)
    gu, dn = (160, 256), (128, D)
    V, dma = pltpu.VMEM, pltpu.SemaphoreType.DMA
    scratch = [
        V((2, tokens, D), BF), V((2, D, tokens), BF), V((tokens, D), BF), V((D, tokens), BF), V((tokens, D), BF), V((tokens, D), F32),
        V((tokens, 256), BF), V((tokens, 256), BF), V((tokens, 256), BF),
        V((2, D, 256), BF), V((2, D, 256), BF), V((2, 256, D), BF), V((D, 256), F32), V((D, 256), F32), V((D, 256), F32),
        V((HELD, 4, *gu), F32), V((HELD, *dn), F32), V((2, 4, *gu), BF), V((2, *dn), BF), V((SLOTS, 4, *gu), BF), V((SLOTS, *dn), BF),
        V((2, 3, *gu), BF), V((2, *dn), BF), V((2, 3, *gu), BF), V((2, *dn), BF),
        V((SLOTS, 3, *gu), BF), V((SLOTS, *dn), BF), V((SLOTS, 3, *gu), BF), V((SLOTS, *dn), BF),
        V((2, *gu), BF), V((2, *dn), BF), V(block, BF), V(block, BF), V(down, BF),
        dma((2, 6)), dma((5,)), dma((2, 2)), dma((SLOTS, 2)), dma((2, 4)), dma((SLOTS, 4)), dma((2, 4)), dma((SLOTS, 4)),
        dma((2, 2)), dma((2, 3, 2)), dma((2, 3, 2)), dma((3, 2, 4, 2)), dma((SLOTS, 3, 2)), dma((SLOTS, 3, 2)), dma((3, SLOTS, 4, 2)),
        *[V(s, F32) for s in (block, block, down)] * 2, dma((6,)),
    ]
    return pl.pallas_call(
        functools.partial(kernel, tile),
        out_shape=[sds(wide, BF), sds(wide, BF), sds(tall, BF)] + [sds(s, F32) for s in (block, block, down)] * 2,
        in_specs=[hbm] * 11,
        out_specs=[hbm] * 9,
        scratch_shapes=scratch,
        compiler_params=pltpu.CompilerParams(collective_id=0, has_side_effects=True, vmem_limit_bytes=64 * 2**20),
        name="step",
    )


def solution(mesh):
    def step(x, dy, wg, wu, wd, *moments):
        return tuple(step_kernel(x.shape[1])(x[0], dy[0], wg, wu, wd, *moments))

    mine, whole, rows = P(("rep", "dp"), None, None), P(None, None, None), P(None, "dp", None)
    return jax.shard_map(
        step, mesh=mesh, in_specs=(mine, mine) + (whole,) * 3 + (rows,) * 6,
        out_specs=(P("rep", None, None),) * 3 + (P("rep", "dp", None),) * 6, check_vma=False,
    )
```

```python
import functools

import jax
import jax.numpy as jnp
from jax import lax
from jax.experimental import pallas as pl
from jax.experimental.pallas import tpu as pltpu
from jax.sharding import PartitionSpec as P

D, FF, CHUNKS = 640, 2048, 16
BF, F32 = jnp.bfloat16, jnp.float32
SLOTS = 4
HELD = 5


def dot(a, b):
    return lax.dot_general(a, b, (((1,), (0,)), ((), ())), preferred_element_type=F32)


def dot_t(a, b):
    return lax.dot_general(a, b, (((1,), (1,)), ((), ())), preferred_element_type=F32)


def where(j):
    layer, h = 1 - j // 8, j % 2
    c1 = chip_of(j, 0) * 512 + h * 128
    c2 = chip_of(j, 1) * 512 + 256 + h * 128
    return layer, h, pl.multiple_of(c1, 128), pl.multiple_of(c2, 128)


def chip_of(j, core):
    s = (j // 2 + 3 - 2 * (j // 8)) % 4
    return s + core * (3 - 2 * s)


def adam(w, m, v, g):
    m = 0.9 * m + 0.1 * g
    v = 0.95 * v + 0.05 * g * g
    return (w - 0.02 * (m * lax.rsqrt(v + 1e-8) + 0.1 * w)).astype(BF), m, v


def kernel(tile, x, dy, wg, wu, wd, *refs):
    moments, (ng, nu, nd), new_moments, (a_s, at_s, do_s, dot_s, h_s, da_s, act_s, dg_s, du_s, wgb, wub, wdb, gg, gu, gd,
           pg, pd, d2s_g, d2s_d, d2r_g, d2r_d, sr_g, sr_d, sl_g, sl_d, rl_g, rl_d, rr_g, rr_d, nw_g, nw_d,
           og, ou, od, wsem, lsem, d2_ss, d2_rs, sr_ss, rl_rs, sl_ss, rr_rs, own_s, ar_ss, al_ss, ap_ss, al_rs, ar_rs, ap_rs,
           mg, mu, md, vg, vu, vd, msem) = refs[:6], refs[6:9], refs[9:15], refs[15:]
    held = (mg, mu, md, vg, vu, vd)
    dev = lax.axis_index("dp")
    z, k = dev // 2, dev % 2
    right, left, other = {"dp": (dev + 2) % 8}, {"dp": (dev + 6) % 8}, {"dp": z * 2 + 1 - k}
    tiles = h_s.shape[0] // tile

    barrier = pltpu.get_barrier_semaphore()
    for to in (right, left, other):
        pl.semaphore_signal(barrier, inc=1, device_id=to, device_id_type=pl.DeviceIdType.MESH)
    pl.semaphore_wait(barrier, 3)

    def remote(src, dst, ss, rs, to):
        return pltpu.make_async_remote_copy(src_ref=src, dst_ref=dst, send_sem=ss, recv_sem=rs, device_id=to,
                                            device_id_type=pl.DeviceIdType.MESH)

    def ok(j):
        return (j >= 0) & (j < CHUNKS)

    def weights(j):
        layer, _, c1, c2 = where(j)
        slot = j % 2
        out = []
        for i, c in enumerate((c1, c2)):
            here = slice(128 * i, 128 * i + 128)
            out.append((wg.at[layer, :, pl.ds(c, 128)], wgb.at[slot, :, here]))
            out.append((wu.at[layer, :, pl.ds(c, 128)], wub.at[slot, :, here]))
            out.append((wd.at[layer, pl.ds(c, 128), :], wdb.at[slot, here, :]))
        return [pltpu.make_async_copy(src, dst, wsem.at[slot, i]) for i, (src, dst) in enumerate(out)]

    def over_tiles(body):
        @pl.loop(0, tiles)
        def _(i):
            body(pl.ds(pl.multiple_of(i * tile, tile), tile))

    def unit(h):
        return lax.rsqrt(jnp.mean(h * h, -1, keepdims=True) + 1e-6)

    here = pltpu.make_async_copy(x, h_s, lsem.at[0])
    mine = pl.ds(pl.multiple_of(80 * dev, 16), 80)
    later = [pltpu.make_async_copy(wg.at[:, mine, :], og, lsem.at[2]), pltpu.make_async_copy(wu.at[:, mine, :], ou, lsem.at[3]),
             pltpu.make_async_copy(wd.at[:, pl.ds(pl.multiple_of(256 * dev, 256), 256), :], od, lsem.at[4]),
             pltpu.make_async_copy(dy, do_s, lsem.at[1])]
    later += [pltpu.make_async_copy(src, dst, msem.at[i]) for i, (src, dst) in enumerate(zip(moments, held, strict=True))]
    for c in [here] + weights(8) + later:
        c.start()
    here.wait()

    def enter(rows):
        h = h_s[rows, :].astype(F32)
        a_s[0, rows, :] = (h * unit(h)).astype(BF)
        da_s[rows, :] = jnp.zeros((tile, D), F32)

    over_tiles(enter)

    @pl.loop(8, 16)
    def _(j):
        slot = j % 2
        for c in weights(j):
            c.wait()
        for c in weights((j + 1) % 16):
            c.start()

        def forward(rows):
            a = a_s[0, rows, :]
            gate, up = dot(a, wgb[slot]), dot(a, wub[slot])
            da_s[rows, :] += dot((gate * jax.nn.sigmoid(gate) * up).astype(BF), wdb[slot])

        over_tiles(forward)

    def leave(rows):
        h = (h_s[rows, :].astype(F32) + da_s[rows, :].astype(BF).astype(F32)).astype(BF)
        h_s[rows, :] = h
        h = h.astype(F32)
        a_s[1, rows, :] = (h * unit(h)).astype(BF)
        at_s[1, :, rows] = a_s[1, rows, :].T
        dot_s[:, rows] = do_s[rows, :].T
        da_s[rows, :] = jnp.zeros((tile, D), F32)

    for c in later:
        c.wait()
    over_tiles(leave)

    def chunk(t):
        slot, layer = t % 2, 1 - t // 8

        @pl.when(t == 8)
        def _():
            def back(rows):
                h = h_s[rows, :].astype(F32)
                da = da_s[rows, :].astype(BF).astype(F32)
                r = unit(h)
                dh = r * da - h * (r * r * r * jnp.mean(h * da, -1, keepdims=True))
                do_s[rows, :] = (do_s[rows, :].astype(F32) + dh.astype(BF).astype(F32)).astype(BF)
                dot_s[:, rows] = do_s[rows, :].T

            over_tiles(back)

        @pl.when(t == 4)
        def _():
            def turn(rows):
                at_s[0, :, rows] = a_s[0, rows, :].T

            over_tiles(turn)

        for c in weights(t):
            c.wait()

        @pl.when(t + 1 < CHUNKS)
        def _():
            for c in weights(t + 1):
                c.start()

        def through(rows):
            a, d = a_s[layer, rows, :], do_s[rows, :]
            gate, up = dot(a, wgb[slot]), dot(a, wub[slot])
            dact = dot_t(d, wdb[slot]).astype(BF).astype(F32)
            sig = jax.nn.sigmoid(gate)
            silu = gate * sig
            act_s[rows, :] = (silu * up).astype(BF)
            du_s[rows, :] = (dact * silu).astype(BF)
            dg_s[rows, :] = (dact * up * (sig * (1 + gate * (1 - sig)))).astype(BF)

        over_tiles(through)

    def inward(t):
        slot = t % 2

        @pl.when(t < 8)
        def _():
            def into(rows):
                da_s[rows, :] += dot_t(dg_s[rows, :], wgb[slot]) + dot_t(du_s[rows, :], wub[slot])

            over_tiles(into)

    def gradients(t):
        slot, keep, layer = t % 2, t % HELD, 1 - t // 8
        gg[...] = dot(at_s[layer], dg_s[...])
        gu[...] = dot(at_s[layer], du_s[...])
        gd[...] = dot(dot_s[...], act_s[...])
        for b in range(4):
            mine = pl.ds(pl.multiple_of(160 * b + 80 * k, 16), 80)
            its = pl.ds(pl.multiple_of(160 * b + 80 * (1 - k), 16), 80)
            for i, g in enumerate((gg, gu)):
                pg[keep, b, 80 * i : 80 * i + 80, :] = g[mine, :]
                d2s_g[slot, b, 80 * i : 80 * i + 80, :] = g[its, :].astype(BF)
        pd[keep] = gd[:, pl.ds(pl.multiple_of(128 * k, 128), 128)].T
        d2s_d[slot] = gd[:, pl.ds(pl.multiple_of(128 * (1 - k), 128), 128)].T.astype(BF)
        for c in swap(t):
            c.start()

    def swap(j):
        slot, keep = j % 2, j % SLOTS
        return [remote(d2s_g.at[slot], d2r_g.at[keep], d2_ss.at[slot, 0], d2_rs.at[keep, 0], other),
                remote(d2s_d.at[slot], d2r_d.at[keep], d2_ss.at[slot, 1], d2_rs.at[keep, 1], other)]

    def to_right(j, b):
        return remote(sr_g.at[j % 2, b - 1], rl_g.at[j % SLOTS, b - 1], sr_ss.at[j % 2, b - 1], rl_rs.at[j % SLOTS, b - 1], right)

    def to_right_d(j):
        return remote(sr_d.at[j % 2], rl_d.at[j % SLOTS], sr_ss.at[j % 2, 3], rl_rs.at[j % SLOTS, 3], right)

    def to_left(j, b):
        return remote(sl_g.at[j % 2, b], rr_g.at[j % SLOTS, b], sl_ss.at[j % 2, b], rr_rs.at[j % SLOTS, b], left)

    def to_left_d(j):
        return remote(sl_d.at[j % 2], rr_d.at[j % SLOTS], sl_ss.at[j % 2, 3], rr_rs.at[j % SLOTS, 3], left)

    def reduce(t):
        j = t - 1

        @pl.when(ok(j))
        def _():
            for c in swap(j):
                c.wait()
            keep, came = j % HELD, j % SLOTS
            for b in range(4):
                pg[keep, b] += d2r_g[came, b].astype(F32)
            pd[keep] += d2r_d[came].astype(F32)

        jr, jl = t - 1 - z, t - 4 + z
        sr, sl = chip_of(jr, k), chip_of(jl, k)

        def rightward(b):
            @pl.when(ok(jr) & (z > 0) & (z <= b))
            def _():
                to_right(jr, b).wait_recv()
                pg[jr % HELD, b] += rl_g[jr % SLOTS, b - 1].astype(F32)

            @pl.when(ok(jr) & (z < b))
            def _():
                sr_g[jr % 2, b - 1] = pg[jr % HELD, b].astype(BF)
                to_right(jr, b).start()

            @pl.when(ok(jr - 1) & (z < b))
            def _():
                to_right(jr - 1, b).wait_send()

        def leftward(b):
            @pl.when(ok(jl) & (z < 3) & (z >= b))
            def _():
                to_left(jl, b).wait_recv()
                pg[jl % HELD, b] += rr_g[jl % SLOTS, b].astype(F32)

            @pl.when(ok(jl) & (z > b))
            def _():
                sl_g[jl % 2, b] = pg[jl % HELD, b].astype(BF)
                to_left(jl, b).start()

            @pl.when(ok(jl - 1) & (z > b))
            def _():
                to_left(jl - 1, b).wait_send()

        for b in (3, 2, 1):
            rightward(b)
            leftward(3 - b)

        @pl.when(ok(jr) & (z > 0) & (z <= sr))
        def _():
            to_right_d(jr).wait_recv()
            pd[jr % HELD] += rl_d[jr % SLOTS].astype(F32)

        @pl.when(ok(jr) & (z < sr))
        def _():
            sr_d[jr % 2] = pd[jr % HELD].astype(BF)
            to_right_d(jr).start()

        @pl.when(ok(jr - 1) & (z < chip_of(jr - 1, k)))
        def _():
            to_right_d(jr - 1).wait_send()

        @pl.when(ok(jl) & (z < 3) & (z >= sl))
        def _():
            to_left_d(jl).wait_recv()
            pd[jl % HELD] += rr_d[jl % SLOTS].astype(F32)

        @pl.when(ok(jl) & (z > sl))
        def _():
            sl_d[jl % 2] = pd[jl % HELD].astype(BF)
            to_left_d(jl).start()

        @pl.when(ok(jl - 1) & (z > chip_of(jl - 1, k)))
        def _():
            to_left_d(jl - 1).wait_send()

    def update(j):
        layer, h, c1, c2 = where(j)
        keep, slot = j % HELD, j % 2
        for i, (w, m, v) in enumerate(((og, mg, vg), (ou, mu, vu))):
            for n, c in enumerate((c1, c2)):
                at = (layer, slice(None), pl.ds(c, 128))
                g = pg[keep, z, 80 * i : 80 * i + 80, 128 * n : 128 * n + 128].astype(BF).astype(F32)
                new, m[at], v[at] = adam(w[at].astype(F32), m[at], v[at], g)
                nw_g[slot, 80 * i : 80 * i + 80, 128 * n : 128 * n + 128] = new

        @pl.when(chip_of(j, k) == z)
        def _():
            at = (layer, pl.ds(pl.multiple_of(h * 128, 128), 128), slice(None))
            g = pd[keep].astype(BF).astype(F32)
            new, md[at], vd[at] = adam(od[at].astype(F32), md[at], vd[at], g)
            nw_d[slot] = new

    def windows(j, origin, core):
        layer, h, c1, c2 = where(j)
        rows = pl.ds(pl.multiple_of(160 * origin + 80 * core, 16), 80)
        down = pl.ds(pl.multiple_of((2 * origin + core) * 256 + 128 * h, 128), 128)
        return [n.at[layer, rows, pl.ds(c, 128)] for n in (ng, nu) for c in (c1, c2)], nd.at[layer, down, :], chip_of(j, core) == origin

    def sources(j, a, origin):
        if a == 0:
            slot = j % 2
            return [nw_g.at[slot, 80 * i : 80 * i + 80, 128 * n : 128 * n + 128] for i in range(2) for n in range(2)], nw_d.at[slot]
        return windows(j, origin, k)[:2]

    def start(j, a, origin, ss, rs, to):
        into, into_d, has = windows(j, origin, k)
        src, src_d = sources(j, a, origin)
        for x, y in zip(src, into, strict=True):
            remote(x, y, ss.at[j % 2, a, 0], rs.at[j % SLOTS, a, 0], to).start()

        @pl.when(has)
        def _():
            remote(src_d, into_d, ss.at[j % 2, a, 1], rs.at[j % SLOTS, a, 1], to).start()

    def finish(has, gate_up, down):
        pltpu.make_async_copy(nw_g.at[0], nw_g.at[0], gate_up).wait()

        @pl.when(has)
        def _():
            pltpu.make_async_copy(nw_d.at[0], nw_d.at[0], down).wait()

    def gather(t):
        def each(j, a, origin, side, what):
            valid = ok(j) & (origin >= 0) & (origin < 4)
            has = chip_of(j, k) == origin

            @pl.when(valid)
            def _():
                if side in (0, 1) and a < 3:
                    pl.when(z < 3)(lambda: what(j, a, origin, has, ar_ss, al_rs, right))
                if side in (0, 2) and a < 3:
                    pl.when(z > 0)(lambda: what(j, a, origin, has, al_ss, ar_rs, left))
                what(j, a, origin, has, ap_ss.at[side], ap_rs.at[side], other)

        def waited(j, a, origin, has, ss, rs, to):
            finish(has, ss.at[j % 2, a, 0], ss.at[j % 2, a, 1])

        def begun(j, a, origin, has, ss, rs, to):
            start(j, a, origin, ss, rs, to)

        j = t - 4

        @pl.when(ok(j - 1))
        def _():
            finish(chip_of(j - 1, k) == z, own_s.at[(j - 1) % 2, 0], own_s.at[(j - 1) % 2, 1])

        each(j - 1, 0, z, 0, waited)

        @pl.when(ok(j))
        def _():
            update(j)
            into, into_d, has = windows(j, z, k)
            src, src_d = sources(j, 0, z)
            for x, y in zip(src, into, strict=True):
                pltpu.make_async_copy(x, y, own_s.at[j % 2, 0]).start()

            @pl.when(has)
            def _():
                pltpu.make_async_copy(src_d, into_d, own_s.at[j % 2, 1]).start()

        each(j, 0, z, 0, begun)

        for a in (1, 2, 3):
            ja = t - 4 - a
            for side, origin, rs in ((1, z - a, al_rs), (2, z + a, ar_rs)):
                each(ja - 1, a, origin, side, waited)

                @pl.when(ok(ja) & (origin >= 0) & (origin < 4))
                def _():
                    finish(chip_of(ja, k) == origin, rs.at[ja % SLOTS, a - 1, 0], rs.at[ja % SLOTS, a - 1, 1])

                each(ja, a, origin, side, begun)

        for a in (0, 1, 2, 3):
            jp = t - 5 - a
            for side, origin in ((0, z),) if a == 0 else ((1, z - a), (2, z + a)):
                @pl.when(ok(jp) & (origin >= 0) & (origin < 4))
                def _():
                    finish(chip_of(jp, 1 - k) == origin, ap_rs.at[side, jp % SLOTS, a, 0], ap_rs.at[side, jp % SLOTS, a, 1])

    back_out = [pltpu.make_async_copy(src, dst, msem.at[i]) for i, (src, dst) in enumerate(zip(held, new_moments, strict=True))]

    @pl.loop(0, CHUNKS + 8)
    def _(t):
        pl.when(t < CHUNKS)(lambda: chunk(t))
        reduce(t)
        pl.when(t < 8)(lambda: inward(t))
        pl.when(t < CHUNKS)(lambda: gradients(t))
        gather(t)

        @pl.when(t == CHUNKS + 3)
        def _():
            for c in back_out:
                c.start()

    for c in back_out:
        c.wait()


def step_kernel(tokens):
    tile = min(tokens, 1024)
    sds = jax.ShapeDtypeStruct
    hbm = pl.BlockSpec(memory_space=pltpu.HBM)
    wide, tall, block, down = (2, D, FF), (2, FF, D), (2, D // 8, FF), (2, FF // 8, D)
    gu, dn = (160, 256), (128, D)
    V, dma = pltpu.VMEM, pltpu.SemaphoreType.DMA
    scratch = [
        V((2, tokens, D), BF), V((2, D, tokens), BF), V((tokens, D), BF), V((D, tokens), BF), V((tokens, D), BF), V((tokens, D), F32),
        V((tokens, 256), BF), V((tokens, 256), BF), V((tokens, 256), BF),
        V((2, D, 256), BF), V((2, D, 256), BF), V((2, 256, D), BF), V((D, 256), F32), V((D, 256), F32), V((D, 256), F32),
        V((HELD, 4, *gu), F32), V((HELD, *dn), F32), V((2, 4, *gu), BF), V((2, *dn), BF), V((SLOTS, 4, *gu), BF), V((SLOTS, *dn), BF),
        V((2, 3, *gu), BF), V((2, *dn), BF), V((2, 3, *gu), BF), V((2, *dn), BF),
        V((SLOTS, 3, *gu), BF), V((SLOTS, *dn), BF), V((SLOTS, 3, *gu), BF), V((SLOTS, *dn), BF),
        V((2, *gu), BF), V((2, *dn), BF), V(block, BF), V(block, BF), V(down, BF),
        dma((2, 6)), dma((5,)), dma((2, 2)), dma((SLOTS, 2)), dma((2, 4)), dma((SLOTS, 4)), dma((2, 4)), dma((SLOTS, 4)),
        dma((2, 2)), dma((2, 3, 2)), dma((2, 3, 2)), dma((3, 2, 4, 2)), dma((SLOTS, 3, 2)), dma((SLOTS, 3, 2)), dma((3, SLOTS, 4, 2)),
        *[V(s, F32) for s in (block, block, down)] * 2, dma((6,)),
    ]
    return pl.pallas_call(
        functools.partial(kernel, tile),
        out_shape=[sds(wide, BF), sds(wide, BF), sds(tall, BF)] + [sds(s, F32) for s in (block, block, down)] * 2,
        in_specs=[hbm] * 11,
        out_specs=[hbm] * 9,
        scratch_shapes=scratch,
        compiler_params=pltpu.CompilerParams(collective_id=0, has_side_effects=True, vmem_limit_bytes=64 * 2**20),
        name="step",
    )


def solution(mesh):
    def step(x, dy, wg, wu, wd, *moments):
        return tuple(step_kernel(x.shape[1])(x[0], dy[0], wg, wu, wd, *moments))

    mine, whole, rows = P(("rep", "dp"), None, None), P(None, None, None), P(None, "dp", None)
    return jax.shard_map(
        step, mesh=mesh, in_specs=(mine, mine) + (whole,) * 3 + (rows,) * 6,
        out_specs=(P("rep", None, None),) * 3 + (P("rep", "dp", None),) * 6, check_vma=False,
    )
```
